32 devices in a mesh: dp: 4 (over x, y), tp: 8 (over z, core).
Axes of the slice: x: 2, y: 2, z: 4, core: 2. Of those that a mesh axis runs over, the one named last changes fastest.
Arguments:
- x: bfloat16 [11264, 3072], P(('dp', 'tp')), parts along dimension 0
- dy: bfloat16 [11264, 3072], P(('dp', 'tp')), parts along dimension 0
- pre: bfloat16 [11264, 9216], P('dp', 'tp'), parts along dimension 0
- w_in: bfloat16 [3072, 9216], P(None, 'tp')
- w_down: bfloat16 [9216, 3072], P('tp')
Outputs:
- output 1: bfloat16 [11264, 3072], P(('dp', 'tp')), parts along dimension 0
- output 2: bfloat16 [12288, 9216], P('dp', 'tp'), parts along dimension 0
- output 3: bfloat16 [36864, 3072], P(('dp', 'tp')), parts along dimension 0
There are 4 independent parts. The reference program is written for one: setup_inputs(seed, part) draws one part's arguments, and reference() takes and returns one part's arrays. A program takes and returns all parts, laid end to end along the dimension named above; an argument that names none is the same for every part.
All inputs are finite; a program needn't handle non-finite values.
Results may differ from the reference program's by a relative error of at most 0.012.
Values are sent between devices in bfloat16 or wider.
A program may use at most 2 GiB of HBM per device.

```python
import jax
import jax.numpy as jnp

ROWS = 2816
D = 3072
FF = 9216


def act(pre):
    return jnp.square(jax.nn.relu(pre))


def setup_inputs(seed: int = 0, part: int = 0) -> dict:
    kx, ky, ka, ki, kd = jax.random.split(jax.random.key(seed), 5)
    kx, ky, ka = (jax.random.fold_in(k, part) for k in (kx, ky, ka))
    drawn = {
        "x": jax.random.normal(kx, (ROWS, D), jnp.float32),
        "dy": jax.random.normal(ky, (ROWS, D), jnp.float32),
        "pre": jax.random.normal(ka, (ROWS, FF), jnp.float32),
        "w_in": jax.random.normal(ki, (D, FF), jnp.float32) * D**-0.5,
        "w_down": jax.random.normal(kd, (FF, D), jnp.float32) * FF**-0.5,
    }
    return {k: v.astype(jnp.bfloat16) for k, v in drawn.items()}


def reference(x, dy, pre, w_in, w_down):
    hidden, back = jax.vjp(act, pre.astype(jnp.float32))
    d_hidden = jnp.dot(dy, w_down.T, preferred_element_type=jnp.float32)
    d_pre = back(d_hidden)[0].astype(jnp.bfloat16)
    dx = jnp.dot(d_pre, w_in.T, preferred_element_type=jnp.float32)
    dw_in = jnp.dot(x.T, d_pre, preferred_element_type=jnp.float32)
    dw_down = jnp.dot(hidden.astype(jnp.bfloat16).T, dy, preferred_element_type=jnp.float32)
    return tuple(g.astype(jnp.bfloat16) for g in (dx, dw_in, dw_down))
```

```python
import functools

import jax
import jax.numpy as jnp
from jax import lax
from jax.experimental import pallas as pl
from jax.experimental.pallas import tpu as pltpu
from jax.sharding import PartitionSpec as P

MESH = pl.DeviceIdType.MESH
F32, BF16 = jnp.float32, jnp.bfloat16
NT = (((1,), (1,)), ((), ()))
CHIPS = 4


def tile(n):
    return next(t for t in (384, 256, 128) if n % t == 0)


def kernel(
    dy_ref, x_ref, pre_ref, wi_ref, wd_ref,
    dyf_ref, xf_ref, dpre_ref, finl_ref, finr_ref, own_ref,
    wd_v, wi_v, dp_v, dyb, preb, prt_v, lin_v, out_v, rs_v, fin_v, own_v,
    link_s, link_r, d2d_s, d2d_r, push_s, push_r, rs_s, rs_r, load_s, dpre_s, misc_s,
):
    me = lax.axis_index("tp")
    g = lax.axis_index("dp")
    z, c = me // 2, me % 2
    rows, d_model = dy_ref.shape
    half = rows // 2
    ff = wd_ref.shape[0]
    ins, fulls = (dy_ref, x_ref), (dyf_ref, xf_ref)
    first, last = z == 0, z == CHIPS - 1
    end, mid = (z == 0) | (z == 3), (z == 1) | (z == 2)
    partner = 2 * z + 1 - c

    def block(zb, core):
        return pl.ds(pl.multiple_of((2 * zb + core) * rows, 16), rows)

    def half_of(zb, core, h):
        return pl.ds(pl.multiple_of((2 * zb + core) * rows + h * half, 16), half)

    def neighbour(d):
        return 2 * (z - 1 if d == 0 else z + 1) + c

    def link(a, d, s, h, zb, own=False, to=None):
        dst = fulls[a].at[half_of(zb, c, h)]
        src = ins[a].at[pl.ds(h * half, half)] if own else dst
        return pltpu.make_async_remote_copy(
            src_ref=src, dst_ref=dst, send_sem=link_s.at[a, d, s, h], recv_sem=link_r.at[a, d, s, h],
            device_id=(g, neighbour(d) if to is None else to), device_id_type=MESH)

    def d2d(a, zb, h, own=False, core=None):
        core = c if core is None else core
        dst = fulls[a].at[half_of(zb, core, h)]
        src = ins[a].at[pl.ds(h * half, half)] if own else dst
        return pltpu.make_async_remote_copy(
            src_ref=src, dst_ref=dst, send_sem=d2d_s.at[a, zb, h], recv_sem=d2d_r.at[a, zb, h],
            device_id=(g, partner), device_id_type=MESH)

    def has_link(d):
        return z >= 1 if d == 0 else z <= 2

    def arrives(d, s):
        return z + s + 1 <= 3 if d == 0 else z - s - 1 >= 0

    def source(d, s):
        return z + s + 1 if d == 0 else z - s - 1

    def arrival(a, d, s, h):
        zb = source(d, s)
        link(a, d, s, h, zb, to=partner).wait_recv()
        if s < 2:
            @pl.when(has_link(d))
            def _():
                link(a, d, s + 1, h, zb).start()
        d2d(a, zb, h).start()

    def send_own(a, d):
        for h in range(2):
            link(a, d, 0, h, z, own=True).start()

    def push(zb):
        return pltpu.make_async_remote_copy(
            src_ref=out_v, dst_ref=prt_v.at[zb], send_sem=push_s, recv_sem=push_r.at[zb],
            device_id=(g, partner), device_id_type=MESH)

    def rs(d, s, to):
        return pltpu.make_async_remote_copy(
            src_ref=rs_v.at[s - 2], dst_ref=lin_v.at[d, s - 2], send_sem=rs_s.at[s - 2], recv_sem=rs_r.at[d, s - 2],
            device_id=(g, to), device_id_type=MESH)

    def local(src, dst, sem):
        return pltpu.make_async_copy(src, dst, sem)

    def dpre_block(slot, b):
        t = tile(ff)
        at = pl.ds(pl.multiple_of(b * rows, 16), rows)

        def body(j, _):
            cols = pl.ds(pl.multiple_of(j * t, 128), t)
            dh = lax.dot_general(dyb[slot], wd_v[cols, :], NT, preferred_element_type=F32)
            p = preb[slot, :, cols].astype(F32)
            dp_v[at, cols] = jnp.where(p > 0, dh * (2.0 * p), 0.0).astype(BF16)
            return 0

        lax.fori_loop(0, ff // t, body, 0)

    def dx_block(b, store, adds):
        t = tile(d_model)
        at = pl.ds(pl.multiple_of(b * rows, 16), rows)

        def body(j, _):
            cols = pl.ds(pl.multiple_of(j * t, 128), t)
            acc = lax.dot_general(dp_v[at, :], wi_v[cols, :], NT, preferred_element_type=F32)
            for add in adds:
                acc = acc + add[:, cols].astype(F32)
            store[:, cols] = acc.astype(store.dtype)
            return 0

        lax.fori_loop(0, d_model // t, body, 0)

    def dpre_out(b):
        at = pl.ds(pl.multiple_of(b * rows, 16), rows)
        return local(dp_v.at[at], dpre_ref.at[at], dpre_s.at[b])

    def load(slot, zb, core, src=None):
        at = block(zb, core)
        return (local(dyf_ref.at[at] if src is None else src, dyb.at[slot], load_s.at[slot, 0]),
                local(pre_ref.at[at], preb.at[slot], load_s.at[slot, 1]))

    def process(zb, own=False):
        for copy in load(0, zb, c, dy_ref if own else None):
            copy.start()
        for h in range(2):
            d2d(0, zb, h, core=1 - c).wait_recv()
        for copy in load(1, zb, 1 - c):
            copy.start()
        if own:
            local(wd_ref, wd_v, misc_s.at[0]).wait()
        for slot in range(2):
            for copy in load(slot, zb, c if slot == 0 else 1 - c, dy_ref if own and slot == 0 else None):
                copy.wait()
            b = 2 * zb + (c if slot == 0 else 1 - c)
            dpre_block(slot, b)
            dpre_out(b).start()
        if own:
            local(dyb.at[0], dyf_ref.at[block(z, c)], misc_s.at[2]).start()
            local(wi_ref, wi_v, misc_s.at[1]).wait()
            local(dyb.at[0], dyf_ref.at[block(z, c)], misc_s.at[2]).wait()
        else:
            push(zb).wait_send()
        dx_block(2 * zb + 1 - c, out_v, ())
        push(zb).start()

    def finish(d):
        for dd, ref in ((0, finl_ref), (1, finr_ref)):
            @pl.when(d == dd)
            def _():
                copy = local(fin_v, ref, misc_s.at[3])
                copy.start()
                copy.wait()

    main = jnp.where(z >= 2, 0, 1)
    other = 1 - main

    def chip_at(d, s):
        return z + s * (2 * d - 1)

    def sum_at(d, s, lin):
        zb = chip_at(d, s)
        push(zb).wait_recv()
        adds = [prt_v.at[zb]]
        if lin:
            rs(d, s + 1, partner).wait_recv()
            adds.append(lin_v.at[d, s - 1])
        dx_block(2 * zb + c, fin_v if s == 1 else rs_v.at[s - 2], adds)
        if s == 1:
            finish(d)
        else:
            rs(d, s, 2 * chip_at(d, 1) + c).start()

    barrier = pltpu.get_barrier_semaphore()
    pl.semaphore_signal(barrier, inc=1, device_id=(g, partner), device_id_type=MESH)
    for d in range(2):
        @pl.when(has_link(d))
        def _():
            pl.semaphore_signal(barrier, inc=1, device_id=(g, neighbour(d)), device_id_type=MESH)
    pl.semaphore_wait(barrier, jnp.where(end, 2, 3))

    for d in range(2):
        @pl.when(has_link(d))
        def _():
            send_own(0, d)
    for h in range(2):
        d2d(0, z, h, own=True).start()
    local(wd_ref, wd_v, misc_s.at[0]).start()
    local(wi_ref, wi_v, misc_s.at[1]).start()

    @pl.when(last)
    def _():
        send_own(1, 0)

    @pl.when(first)
    def _():
        send_own(1, 1)

    for h in range(2):
        d2d(1, z, h, own=True).start()
    process(z, own=True)
    copy = local(x_ref, fin_v, misc_s.at[3])
    copy.start()
    copy.wait()
    copy = local(fin_v, xf_ref.at[block(z, c)], misc_s.at[3])
    copy.start()
    copy.wait()
    push(z).wait_recv()
    dx_block(2 * z + c, own_v, (prt_v.at[z],))
    local(own_v, own_ref, misc_s.at[4]).start()

    for h in range(2):
        for d in range(2):
            @pl.when(arrives(d, 0))
            def _():
                arrival(0, d, 0, h)

    @pl.when(z == 2)
    def _():
        send_own(1, 0)

    @pl.when(z == 1)
    def _():
        send_own(1, 1)

    def near(i, _):
        process(jnp.where(first, 1, jnp.where(last, 2, z - 1 + 2 * i)))
        return 0

    lax.fori_loop(0, jnp.where(end, 1, 2), near, 0)

    @pl.when(end)
    def _():
        sum_at(main, 1, False)

    for h in range(2):
        for d in range(2):
            @pl.when(arrives(d, 1))
            def _():
                arrival(0, d, 1, h)

    @pl.when(z == 1)
    def _():
        send_own(1, 0)

    @pl.when(z == 2)
    def _():
        send_own(1, 1)

    def x_in(zz, d, s):
        @pl.when(z == zz)
        def _():
            for h in range(2):
                arrival(1, d, s, h)

    process(jnp.where(z < 2, z + 2, z - 2))

    @pl.when(end)
    def _():
        sum_at(main, 2, False)

    x_in(1, 1, 0)
    x_in(2, 0, 0)

    @pl.when(end)
    def _():
        for h in range(2):
            for d in range(2):
                @pl.when(arrives(d, 2))
                def _():
                    arrival(0, d, 2, h)
        process(3 - z)
        sum_at(main, 3, False)

    x_in(1, 0, 0)
    x_in(2, 1, 0)

    @pl.when(mid)
    def _():
        sum_at(main, 1, True)

    x_in(1, 0, 1)
    x_in(2, 1, 1)
    x_in(0, 0, 0)
    x_in(3, 1, 0)

    @pl.when(mid)
    def _():
        sum_at(main, 2, True)

    x_in(0, 0, 1)
    x_in(3, 1, 1)

    @pl.when(mid)
    def _():
        sum_at(other, 1, True)

    x_in(0, 0, 2)
    x_in(3, 1, 2)

    for zb in range(CHIPS):
        for h in range(2):
            d2d(1, zb, h, core=1 - c).wait_recv()
            for a in range(2):
                d2d(a, zb, h).wait_send()
    for a in range(2):
        for d in range(2):
            for s in range(3):
                sent = has_link(d) if s == 0 else has_link(d) & arrives(d, s - 1)

                @pl.when(sent)
                def _():
                    for h in range(2):
                        link(a, d, s, h, z).wait_send()
    push(z).wait_send()
    rs(main, 2, partner).wait_send()

    @pl.when(end)
    def _():
        rs(main, 3, partner).wait_send()

    for b in range(2 * CHIPS):
        dpre_out(b).wait()
    local(own_v, own_ref, misc_s.at[4]).wait()


def gather_and_sum(dy, x, pre, w_in, w_down):
    rows, d_model = dy.shape
    tokens, ff = pre.shape
    out = jax.ShapeDtypeStruct
    dma = pltpu.SemaphoreType.DMA
    flops = 4 * tokens * d_model * ff
    return pl.pallas_call(
        kernel,
        out_shape=(out((tokens, d_model), BF16), out((tokens, d_model), BF16), out((tokens, ff), BF16),
                   out((rows, d_model), BF16), out((rows, d_model), BF16), out((rows, d_model), F32)),
        in_specs=[pl.BlockSpec(memory_space=pl.ANY)] * 5,
        out_specs=(pl.BlockSpec(memory_space=pl.ANY),) * 6,
        scratch_shapes=[
            pltpu.VMEM((ff, d_model), BF16),
            pltpu.VMEM((d_model, ff), BF16),
            pltpu.VMEM((tokens, ff), BF16),
            pltpu.VMEM((2, rows, d_model), BF16),
            pltpu.VMEM((2, rows, ff), BF16),
            pltpu.VMEM((CHIPS, rows, d_model), BF16),
            pltpu.VMEM((2, 2, rows, d_model), BF16),
            pltpu.VMEM((rows, d_model), BF16),
            pltpu.VMEM((2, rows, d_model), BF16),
            pltpu.VMEM((rows, d_model), BF16),
            pltpu.VMEM((rows, d_model), F32),
            dma((2, 2, 3, 2)), dma((2, 2, 3, 2)), dma((2, CHIPS, 2)), dma((2, CHIPS, 2)),
            dma, dma((CHIPS,)), dma((2,)), dma((2, 2)), dma((2, 2)), dma((2 * CHIPS,)), dma((5,)),
        ],
        compiler_params=pltpu.CompilerParams(
            collective_id=0, has_side_effects=True, vmem_limit_bytes=66_000_000),
        cost_estimate=pl.CostEstimate(flops=flops, bytes_accessed=8 * tokens * d_model, transcendentals=0),
        name="gather_and_sum",
    )(dy, x, pre, w_in, w_down)


def solution(mesh):
    def step(x, dy, pre, w_in, w_down):
        dyf, xf, d_pre, fin_l, fin_r, own = gather_and_sum(dy, x, pre, w_in, w_down)
        n = 2 * CHIPS
        from_right = lax.ppermute(fin_l, "tp", [(i, i - 2) for i in range(2, n)])
        from_left = lax.ppermute(fin_r, "tp", [(i, i + 2) for i in range(n - 2)])
        hidden = jnp.square(jax.nn.relu(pre.astype(F32))).astype(BF16)
        over_tokens = (((0,), (0,)), ((), ()))
        dw_in = lax.dot_general(xf, d_pre, over_tokens, preferred_element_type=F32).astype(BF16)
        dw_down = lax.dot_general(hidden, dyf, over_tokens, preferred_element_type=F32).astype(BF16)
        dx = (own + from_right.astype(F32) + from_left.astype(F32)).astype(BF16)
        return dx, dw_in, dw_down

    rows = P(("dp", "tp"), None)
    return jax.shard_map(
        step, mesh=mesh,
        in_specs=(rows, rows, P("dp", "tp"), P(None, "tp"), P("tp", None)),
        out_specs=(rows, P("dp", "tp"), rows), check_vma=False)
```

```python
import functools

import jax
import jax.numpy as jnp
from jax import lax
from jax.experimental import pallas as pl
from jax.experimental.pallas import tpu as pltpu
from jax.sharding import PartitionSpec as P

MESH = pl.DeviceIdType.MESH
F32, BF16 = jnp.float32, jnp.bfloat16
NT = (((1,), (1,)), ((), ()))
TN = (((0,), (0,)), ((), ()))
CHIPS = 4


def tile(n):
    return next(t for t in (384, 256, 128) if n % t == 0)


def kernel(
    dy_ref, x_ref, pre_ref, wi_ref, wd_ref,
    dyf_ref, xf_ref, dpre_ref, fina_ref, finb_ref, own_ref, dwd_ref,
    wd_v, wi_v, dp_v, dyb, preb, prt_v, lin_v, out_v, rs_v, fin_v, acc_v,
    link_s, link_r, d2d_s, d2d_r, push_s, push_r, rs_s, rs_r, load_s, dpre_s, misc_s, dwd_s,
):
    me = lax.axis_index("tp")
    g = lax.axis_index("dp")
    z, c = me // 2, me % 2
    rows, d_model = dy_ref.shape
    short = max(16, rows * 2 // 11 // 16 * 16)
    sizes = ((rows // 2, rows - rows // 2), (rows - short, short))
    ff = wd_ref.shape[0]
    ins, fulls = (dy_ref, x_ref), (dyf_ref, xf_ref)
    first, last = z == 0, z == CHIPS - 1
    end, mid = (z == 0) | (z == 3), (z == 1) | (z == 2)
    partner = 2 * z + 1 - c

    def block(zb, core):
        return pl.ds(pl.multiple_of((2 * zb + core) * rows, 16), rows)

    def half_of(a, zb, core, h):
        return pl.ds(pl.multiple_of((2 * zb + core) * rows + h * sizes[a][0], 16), sizes[a][h])

    def neighbour(d):
        return 2 * (z - 1 if d == 0 else z + 1) + c

    def link(a, d, s, h, zb, own=False, to=None):
        dst = fulls[a].at[half_of(a, zb, c, h)]
        src = ins[a].at[pl.ds(h * sizes[a][0], sizes[a][h])] if own else dst
        return pltpu.make_async_remote_copy(
            src_ref=src, dst_ref=dst, send_sem=link_s.at[a, d, s, h], recv_sem=link_r.at[a, d, s, h],
            device_id=(g, neighbour(d) if to is None else to), device_id_type=MESH)

    def d2d(a, zb, h, own=False, core=None):
        core = c if core is None else core
        dst = fulls[a].at[half_of(a, zb, core, h)]
        src = ins[a].at[pl.ds(h * sizes[a][0], sizes[a][h])] if own else dst
        return pltpu.make_async_remote_copy(
            src_ref=src, dst_ref=dst, send_sem=d2d_s.at[a, zb, h], recv_sem=d2d_r.at[a, zb, h],
            device_id=(g, partner), device_id_type=MESH)

    def has_link(d):
        return z >= 1 if d == 0 else z <= 2

    def arrives(d, s):
        return z + s + 1 <= 3 if d == 0 else z - s - 1 >= 0

    def source(d, s):
        return z + s + 1 if d == 0 else z - s - 1

    def arrival(a, d, s, h):
        zb = source(d, s)
        link(a, d, s, h, zb, to=partner).wait_recv()
        if s < 2:
            @pl.when(has_link(d))
            def _():
                link(a, d, s + 1, h, zb).start()
        d2d(a, zb, h).start()

    def send_own(a, d):
        for h in range(2):
            link(a, d, 0, h, z, own=True).start()

    def push(zb):
        return pltpu.make_async_remote_copy(
            src_ref=out_v, dst_ref=prt_v.at[zb], send_sem=push_s, recv_sem=push_r.at[zb],
            device_id=(g, partner), device_id_type=MESH)

    def rs(d, s, to):
        return pltpu.make_async_remote_copy(
            src_ref=rs_v.at[s - 2], dst_ref=lin_v.at[d, s - 2], send_sem=rs_s.at[s - 2], recv_sem=rs_r.at[d, s - 2],
            device_id=(g, to), device_id_type=MESH)

    def local(src, dst, sem):
        return pltpu.make_async_copy(src, dst, sem)

    def dpre_block(slot, b):
        t = tile(ff)
        at = pl.ds(pl.multiple_of(b * rows, 16), rows)

        def body(j, _):
            cols = pl.ds(pl.multiple_of(j * t, 128), t)
            dh = lax.dot_general(dyb[slot], wd_v[cols, :], NT, preferred_element_type=F32)
            p = preb[slot, :, cols].astype(F32)
            dp_v[at, cols] = jnp.where(p > 0, dh * (2.0 * p), 0.0).astype(BF16)
            return 0

        lax.fori_loop(0, ff // t, body, 0)

    def dx_block(b, store, adds):
        t = tile(d_model)
        at = pl.ds(pl.multiple_of(b * rows, 16), rows)

        def body(j, _):
            cols = pl.ds(pl.multiple_of(j * t, 128), t)
            acc = lax.dot_general(dp_v[at, :], wi_v[cols, :], NT, preferred_element_type=F32)
            for add in adds:
                acc = acc + add[:, cols].astype(F32)
            store[:, cols] = acc.astype(store.dtype)
            return 0

        lax.fori_loop(0, d_model // t, body, 0)

    def dpre_out(b):
        at = pl.ds(pl.multiple_of(b * rows, 16), rows)
        return local(dp_v.at[at], dpre_ref.at[at], dpre_s.at[b])

    def load(slot, zb, core, src=None):
        at = block(zb, core)
        return (local(dyf_ref.at[at] if src is None else src, dyb.at[slot], load_s.at[slot, 0]),
                local(pre_ref.at[at], preb.at[slot], load_s.at[slot, 1]))

    def process(zb, own=False):
        for copy in load(0, zb, c, dy_ref if own else None):
            copy.start()
        for h in range(2):
            d2d(0, zb, h, core=1 - c).wait_recv()
        for copy in load(1, zb, 1 - c):
            copy.start()
        if own:
            local(wd_ref, wd_v, misc_s.at[0]).wait()
        for slot in range(2):
            for copy in load(slot, zb, c if slot == 0 else 1 - c, dy_ref if own and slot == 0 else None):
                copy.wait()
            b = 2 * zb + (c if slot == 0 else 1 - c)
            dpre_block(slot, b)
            dpre_out(b).start()
        if own:
            local(dyb.at[0], dyf_ref.at[block(z, c)], misc_s.at[2]).start()
            local(wi_ref, wi_v, misc_s.at[1]).wait()
            local(dyb.at[0], dyf_ref.at[block(z, c)], misc_s.at[2]).wait()
        else:
            push(zb).wait_send()
        dx_block(2 * zb + 1 - c, out_v, ())
        push(zb).start()

    def finish(ref):
        copy = local(fin_v, ref, misc_s.at[3])
        copy.start()
        copy.wait()

    def dw_down_rows(m):
        t, tn = tile(ff), 512 if d_model % 512 == 0 else tile(d_model)
        cols = pl.ds(m * t, t)

        def loads(b, slot):
            at = pl.ds(pl.multiple_of(b * rows, 16), rows)
            return (local(dyf_ref.at[at], dyb.at[slot], load_s.at[slot, 0]),
                    local(pre_ref.at[at, cols], preb.at[slot, :, pl.ds(0, t)], load_s.at[slot, 1]))

        for copy in loads(0, 0):
            copy.start()
        acc_v[...] = jnp.zeros_like(acc_v)

        def token_block(b, _):
            slot = b % 2

            @pl.when(b + 1 < 2 * CHIPS)
            def _():
                for copy in loads(b + 1, 1 - slot):
                    copy.start()

            for copy in loads(b, slot):
                copy.wait()
            hidden = jnp.square(jnp.maximum(preb[slot, :, pl.ds(0, t)].astype(F32), 0.0)).astype(BF16)

            def body(n, _):
                at = pl.ds(pl.multiple_of(n * tn, 128), tn)
                acc_v[:, at] += lax.dot_general(hidden, dyb[slot, :, at], TN, preferred_element_type=F32)
                return 0

            return lax.fori_loop(0, d_model // tn, body, 0)

        lax.fori_loop(0, 2 * CHIPS, token_block, 0)

        def body(n, _):
            at = pl.ds(pl.multiple_of(n * tn, 128), tn)
            wd_v[cols, at] = acc_v[:, at].astype(BF16)
            return 0

        lax.fori_loop(0, d_model // tn, body, 0)
        dw_down_out(m).start()

    def dw_down_out(m):
        at = pl.ds(m * tile(ff), tile(ff))
        return local(wd_v.at[at], dwd_ref.at[at], dwd_s.at[m])

    main = jnp.where(z >= 2, 0, 1)
    other = 1 - main

    def chip_at(d, s):
        return z + s * (2 * d - 1)

    def sum_at(d, s, lin, ref=None):
        zb = chip_at(d, s)
        push(zb).wait_recv()
        adds = [prt_v.at[zb]]
        if lin:
            rs(d, s + 1, partner).wait_recv()
            adds.append(lin_v.at[d, s - 1])
        dx_block(2 * zb + c, fin_v if s == 1 else rs_v.at[s - 2], adds)
        if s == 1:
            finish(ref)
        else:
            rs(d, s, 2 * chip_at(d, 1) + c).start()

    barrier = pltpu.get_barrier_semaphore()
    pl.semaphore_signal(barrier, inc=1, device_id=(g, partner), device_id_type=MESH)
    for d in range(2):
        @pl.when(has_link(d))
        def _():
            pl.semaphore_signal(barrier, inc=1, device_id=(g, neighbour(d)), device_id_type=MESH)
    pl.semaphore_wait(barrier, jnp.where(end, 2, 3))

    for d in range(2):
        @pl.when(has_link(d))
        def _():
            send_own(0, d)
    for h in range(2):
        d2d(0, z, h, own=True).start()
    local(wd_ref, wd_v, misc_s.at[0]).start()
    local(wi_ref, wi_v, misc_s.at[1]).start()

    @pl.when(last)
    def _():
        send_own(1, 0)

    @pl.when(first)
    def _():
        send_own(1, 1)

    for h in range(2):
        d2d(1, z, h, own=True).start()
    process(z, own=True)
    copy = local(x_ref, fin_v, misc_s.at[3])
    copy.start()
    copy.wait()
    copy = local(fin_v, xf_ref.at[block(z, c)], misc_s.at[3])
    copy.start()
    copy.wait()
    push(z).wait_recv()
    own_v = acc_v.at[pl.ds(0, rows)]
    dx_block(2 * z + c, own_v, (prt_v.at[z],))
    local(own_v, own_ref, misc_s.at[4]).start()

    for h in range(2):
        for d in range(2):
            @pl.when(arrives(d, 0))
            def _():
                arrival(0, d, 0, h)

    @pl.when(z == 2)
    def _():
        send_own(1, 0)

    @pl.when(z == 1)
    def _():
        send_own(1, 1)

    def near(i, _):
        process(jnp.where(first, 1, jnp.where(last, 2, z - 1 + 2 * i)))
        return 0

    lax.fori_loop(0, jnp.where(end, 1, 2), near, 0)

    @pl.when(end)
    def _():
        sum_at(main, 1, False, fina_ref)

    for h in range(2):
        for d in range(2):
            @pl.when(arrives(d, 1))
            def _():
                arrival(0, d, 1, h)

    @pl.when(z == 1)
    def _():
        send_own(1, 0)

    @pl.when(z == 2)
    def _():
        send_own(1, 1)

    def x_in(zz, d, s):
        @pl.when(z == zz)
        def _():
            for h in range(2):
                arrival(1, d, s, h)

    process(jnp.where(z < 2, z + 2, z - 2))

    @pl.when(end)
    def _():
        sum_at(main, 2, False)

    x_in(1, 1, 0)
    x_in(2, 0, 0)

    @pl.when(end)
    def _():
        for h in range(2):
            for d in range(2):
                @pl.when(arrives(d, 2))
                def _():
                    arrival(0, d, 2, h)
        process(3 - z)
        sum_at(main, 3, False)

    x_in(1, 0, 0)
    x_in(2, 1, 0)

    @pl.when(mid)
    def _():
        sum_at(main, 1, True, finb_ref)

    local(own_v, own_ref, misc_s.at[4]).wait()
    pieces = list(range(ff // tile(ff)))
    dw_down_rows(pieces.pop(0))

    x_in(1, 0, 1)
    x_in(2, 1, 1)
    x_in(0, 0, 0)
    x_in(3, 1, 0)

    @pl.when(mid)
    def _():
        sum_at(main, 2, True)

    if pieces:
        dw_down_rows(pieces.pop(0))
    x_in(0, 0, 1)
    x_in(3, 1, 1)
    while pieces:
        dw_down_rows(pieces.pop(0))

    @pl.when(mid)
    def _():
        sum_at(other, 1, True, fina_ref)

    x_in(0, 0, 2)
    x_in(3, 1, 2)

    for zb in range(CHIPS):
        for h in range(2):
            d2d(1, zb, h, core=1 - c).wait_recv()
            for a in range(2):
                d2d(a, zb, h).wait_send()
    for a in range(2):
        for d in range(2):
            for s in range(3):
                sent = has_link(d) if s == 0 else has_link(d) & arrives(d, s - 1)

                @pl.when(sent)
                def _():
                    for h in range(2):
                        link(a, d, s, h, z).wait_send()
    push(z).wait_send()
    rs(main, 2, partner).wait_send()

    @pl.when(end)
    def _():
        rs(main, 3, partner).wait_send()

    for b in range(2 * CHIPS):
        dpre_out(b).wait()
    for m in range(ff // tile(ff)):
        dw_down_out(m).wait()


def gather_and_sum(dy, x, pre, w_in, w_down):
    rows, d_model = dy.shape
    tokens, ff = pre.shape
    out = jax.ShapeDtypeStruct
    dma = pltpu.SemaphoreType.DMA
    flops = 6 * tokens * d_model * ff
    return pl.pallas_call(
        kernel,
        out_shape=(out((tokens, d_model), BF16), out((tokens, d_model), BF16), out((tokens, ff), BF16),
                   out((rows, d_model), BF16), out((rows, d_model), BF16), out((rows, d_model), F32),
                   out((ff, d_model), BF16)),
        in_specs=[pl.BlockSpec(memory_space=pl.ANY)] * 5,
        out_specs=(pl.BlockSpec(memory_space=pl.ANY),) * 7,
        scratch_shapes=[
            pltpu.VMEM((ff, d_model), BF16),
            pltpu.VMEM((d_model, ff), BF16),
            pltpu.VMEM((tokens, ff), BF16),
            pltpu.VMEM((2, rows, d_model), BF16),
            pltpu.VMEM((2, rows, ff), BF16),
            pltpu.VMEM((CHIPS, rows, d_model), BF16),
            pltpu.VMEM((2, 2, rows, d_model), BF16),
            pltpu.VMEM((rows, d_model), BF16),
            pltpu.VMEM((2, rows, d_model), BF16),
            pltpu.VMEM((rows, d_model), BF16),
            pltpu.VMEM((max(rows, tile(ff)), d_model), F32),
            dma((2, 2, 3, 2)), dma((2, 2, 3, 2)), dma((2, CHIPS, 2)), dma((2, CHIPS, 2)),
            dma, dma((CHIPS,)), dma((2,)), dma((2, 2)), dma((2, 2)), dma((2 * CHIPS,)), dma((5,)), dma((ff // tile(ff),)),
        ],
        compiler_params=pltpu.CompilerParams(
            collective_id=0, has_side_effects=True, vmem_limit_bytes=66_000_000),
        cost_estimate=pl.CostEstimate(flops=flops, bytes_accessed=8 * tokens * d_model, transcendentals=0),
        name="gather_and_sum",
    )(dy, x, pre, w_in, w_down)


def copy_kernel(src, dst):
    dst[...] = src[...]


def copied(a):
    rows, cols = a.shape
    block = pl.BlockSpec((rows // 9 if rows % 9 == 0 else rows, cols), lambda i: (i, 0))
    return pl.pallas_call(
        copy_kernel, out_shape=jax.ShapeDtypeStruct(a.shape, a.dtype), grid=(9 if rows % 9 == 0 else 1,),
        in_specs=[block], out_specs=block,
        cost_estimate=pl.CostEstimate(flops=rows * cols * 500, bytes_accessed=4 * rows * cols, transcendentals=0),
        compiler_params=pltpu.CompilerParams(vmem_limit_bytes=16_000_000), name="copied")(a)


def solution(mesh):
    def step(x, dy, pre, w_in, w_down):
        _, xf, d_pre, fin_a, fin_b, own, dw_down = gather_and_sum(dy, x, pre, w_in, w_down)
        a = lax.ppermute(fin_a, "tp", [(i, i ^ 2) for i in range(2 * CHIPS)])
        b = lax.ppermute(fin_b, "tp", [(i, i ^ 6) for i in range(2, 6)])
        dw_down = copied(dw_down)
        dw_in = lax.dot_general(xf, d_pre, TN, preferred_element_type=F32).astype(BF16)
        dx = (own + a.astype(F32) + b.astype(F32)).astype(BF16)
        return dx, dw_in, dw_down

    rows = P(("dp", "tp"), None)
    return jax.shard_map(
        step, mesh=mesh,
        in_specs=(rows, rows, P("dp", "tp"), P(None, "tp"), P("tp", None)),
        out_specs=(rows, P("dp", "tp"), rows), check_vma=False)
```

```python
import functools

import jax
import jax.numpy as jnp
from jax import lax
from jax.experimental import pallas as pl
from jax.experimental.pallas import tpu as pltpu
from jax.sharding import PartitionSpec as P

MESH = pl.DeviceIdType.MESH
F32, BF16 = jnp.float32, jnp.bfloat16
NT = (((1,), (1,)), ((), ()))
TN = (((0,), (0,)), ((), ()))
CHIPS = 4


def tile(n):
    return next(t for t in (384, 256, 128) if n % t == 0)


def kernel(
    dy_ref, x_ref, pre_ref, wi_ref, wd_ref,
    dyf_ref, xf_ref, dpre_ref, hi_ref, lo_ref, mid_ref, early_ref, base_ref, dwd_ref,
    wd_v, wi_v, dp_v, dyb, preb, prt_v, lin_v, out_v, rs_v, fin_v, acc_v,
    link_s, link_r, d2d_s, d2d_r, push_s, push_r, rs_s, rs_r, load_s, dpre_s, misc_s, dwd_s,
):
    me = lax.axis_index("tp")
    g = lax.axis_index("dp")
    z, c = me // 2, me % 2
    rows, d_model = dy_ref.shape
    short = max(16, rows * 2 // 11 // 16 * 16)
    part = early_ref.shape[0]
    sizes = ((rows // 2, rows - rows // 2), (rows - short, short))
    ff = wd_ref.shape[0]
    ins, fulls = (dy_ref, x_ref), (dyf_ref, xf_ref)
    first, last = z == 0, z == CHIPS - 1
    end, mid = (z == 0) | (z == 3), (z == 1) | (z == 2)
    partner = 2 * z + 1 - c

    def block(zb, core):
        return pl.ds(pl.multiple_of((2 * zb + core) * rows, 16), rows)

    def half_of(a, zb, core, h):
        return pl.ds(pl.multiple_of((2 * zb + core) * rows + h * sizes[a][0], 16), sizes[a][h])

    def neighbour(d):
        return 2 * (z - 1 if d == 0 else z + 1) + c

    def link(a, d, s, h, zb, own=False, to=None):
        dst = fulls[a].at[half_of(a, zb, c, h)]
        src = ins[a].at[pl.ds(h * sizes[a][0], sizes[a][h])] if own else dst
        return pltpu.make_async_remote_copy(
            src_ref=src, dst_ref=dst, send_sem=link_s.at[a, d, s, h], recv_sem=link_r.at[a, d, s, h],
            device_id=(g, neighbour(d) if to is None else to), device_id_type=MESH)

    def d2d(a, zb, h, own=False, core=None):
        core = c if core is None else core
        dst = fulls[a].at[half_of(a, zb, core, h)]
        src = ins[a].at[pl.ds(h * sizes[a][0], sizes[a][h])] if own else dst
        return pltpu.make_async_remote_copy(
            src_ref=src, dst_ref=dst, send_sem=d2d_s.at[a, zb, h], recv_sem=d2d_r.at[a, zb, h],
            device_id=(g, partner), device_id_type=MESH)

    def has_link(d):
        return z >= 1 if d == 0 else z <= 2

    def arrives(d, s):
        return z + s + 1 <= 3 if d == 0 else z - s - 1 >= 0

    def source(d, s):
        return z + s + 1 if d == 0 else z - s - 1

    def arrival(a, d, s, h):
        zb = source(d, s)
        link(a, d, s, h, zb, to=partner).wait_recv()
        if s < 2:
            @pl.when(has_link(d))
            def _():
                link(a, d, s + 1, h, zb).start()
        d2d(a, zb, h).start()

    def send_own(a, d):
        for h in range(2):
            link(a, d, 0, h, z, own=True).start()

    def push(zb):
        return pltpu.make_async_remote_copy(
            src_ref=out_v, dst_ref=prt_v.at[zb], send_sem=push_s, recv_sem=push_r.at[zb],
            device_id=(g, partner), device_id_type=MESH)

    def rs(k, src=None, to=None):
        dst = {4: lin_v.at[4, pl.ds(part, rows - part)], 5: early_ref}.get(k)
        dst = lin_v.at[k] if dst is None else dst
        return pltpu.make_async_remote_copy(
            src_ref=dst if src is None else src, dst_ref=dst, send_sem=rs_s.at[k], recv_sem=rs_r.at[k],
            device_id=(g, partner if to is None else to), device_id_type=MESH)

    def local(src, dst, sem):
        return pltpu.make_async_copy(src, dst, sem)

    def dpre_block(slot, b):
        t = tile(ff)
        at = pl.ds(pl.multiple_of(b * rows, 16), rows)

        def body(j, _):
            cols = pl.ds(pl.multiple_of(j * t, 128), t)
            dh = lax.dot_general(dyb[slot], wd_v[cols, :], NT, preferred_element_type=F32)
            p = preb[slot, :, cols].astype(F32)
            dp_v[at, cols] = jnp.where(p > 0, dh * (2.0 * p), 0.0).astype(BF16)
            return 0

        lax.fori_loop(0, ff // t, body, 0)

    def dx_block(b, store, adds, tail=None):
        t = tile(d_model)
        at = pl.ds(pl.multiple_of(b * rows, 16), rows)

        def body(j, _):
            cols = pl.ds(pl.multiple_of(j * t, 128), t)
            acc = lax.dot_general(dp_v[at, :], wi_v[cols, :], NT, preferred_element_type=F32)
            for add in adds:
                acc = acc + add[:, cols].astype(F32)
            store[:, cols] = acc.astype(store.dtype)
            if tail is not None:
                store[pl.ds(part, rows - part), cols] += tail[pl.ds(part, rows - part), cols].astype(F32)
            return 0

        lax.fori_loop(0, d_model // t, body, 0)

    def dpre_out(b):
        at = pl.ds(pl.multiple_of(b * rows, 16), rows)
        return local(dp_v.at[at], dpre_ref.at[at], dpre_s.at[b])

    def load(slot, zb, core, src=None):
        at = block(zb, core)
        return (local(dyf_ref.at[at] if src is None else src, dyb.at[slot], load_s.at[slot, 0]),
                local(pre_ref.at[at], preb.at[slot], load_s.at[slot, 1]))

    def process(zb, own=False):
        for copy in load(0, zb, c, dy_ref if own else None):
            copy.start()
        for h in range(2):
            d2d(0, zb, h, core=1 - c).wait_recv()
        for copy in load(1, zb, 1 - c):
            copy.start()
        if own:
            local(wd_ref, wd_v, misc_s.at[0]).wait()
        for slot in range(2):
            for copy in load(slot, zb, c if slot == 0 else 1 - c, dy_ref if own and slot == 0 else None):
                copy.wait()
            b = 2 * zb + (c if slot == 0 else 1 - c)
            dpre_block(slot, b)
            dpre_out(b).start()
        if own:
            local(dyb.at[0], dyf_ref.at[block(z, c)], misc_s.at[2]).start()
            local(wi_ref, wi_v, misc_s.at[1]).wait()
            local(dyb.at[0], dyf_ref.at[block(z, c)], misc_s.at[2]).wait()
        else:
            push(zb).wait_send()
        dx_block(2 * zb + 1 - c, out_v, ())
        push(zb).start()

    def dw_down_rows(m):
        t, tn = tile(ff), 512 if d_model % 512 == 0 else tile(d_model)
        cols = pl.ds(m * t, t)

        def loads(b, slot):
            at = pl.ds(pl.multiple_of(b * rows, 16), rows)
            return (local(dyf_ref.at[at], dyb.at[slot], load_s.at[slot, 0]),
                    local(pre_ref.at[at, cols], preb.at[slot, :, pl.ds(0, t)], load_s.at[slot, 1]))

        for copy in loads(0, 0):
            copy.start()
        acc_v[...] = jnp.zeros_like(acc_v)

        def token_block(b, _):
            slot = b % 2

            @pl.when(b + 1 < 2 * CHIPS)
            def _():
                for copy in loads(b + 1, 1 - slot):
                    copy.start()

            for copy in loads(b, slot):
                copy.wait()
            hidden = jnp.square(jnp.maximum(preb[slot, :, pl.ds(0, t)].astype(F32), 0.0)).astype(BF16)

            def body(n, _):
                at = pl.ds(pl.multiple_of(n * tn, 128), tn)
                acc_v[:, at] += lax.dot_general(hidden, dyb[slot, :, at], TN, preferred_element_type=F32)
                return 0

            return lax.fori_loop(0, d_model // tn, body, 0)

        lax.fori_loop(0, 2 * CHIPS, token_block, 0)

        def body(n, _):
            at = pl.ds(pl.multiple_of(n * tn, 128), tn)
            wd_v[cols, at] = acc_v[:, at].astype(BF16)
            return 0

        lax.fori_loop(0, d_model // tn, body, 0)
        dw_down_out(m).start()

    def dw_down_out(m):
        at = pl.ds(m * tile(ff), tile(ff))
        return local(wd_v.at[at], dwd_ref.at[at], dwd_s.at[m])

    main = jnp.where(z >= 2, 0, 1)
    other = 1 - main

    def chip_at(d, s):
        return z + s * (2 * d - 1)

    def sum_at(d, s, store, lin=None):
        zb = chip_at(d, s)
        push(zb).wait_recv()
        adds = [prt_v.at[zb]]
        if lin is not None:
            rs(lin).wait_recv()
            adds.append(lin_v.at[lin])
        dx_block(2 * zb + c, store, adds)

    def base(adds, tail=None):
        push(z).wait_recv()
        dx_block(2 * z + c, base_v, [prt_v.at[z]] + adds, tail)
        local(base_v, base_ref, misc_s.at[4]).start()

    base_v = acc_v.at[pl.ds(0, rows)]
    onward, back = 2 * chip_at(main, 1) + c, 2 * chip_at(other, 1) + c
    early = c == 1
    hi_copy = local(rs_v.at[1, pl.ds(part, rows - part)], hi_ref, misc_s.at[3])
    lo_copy = local(rs_v.at[1, pl.ds(0, part)], lo_ref, misc_s.at[0])
    mid_copy = local(fin_v.at[pl.ds(0, part)], mid_ref, misc_s.at[1])
    zero_copy = local(out_v.at[pl.ds(0, part)], early_ref, misc_s.at[5])

    barrier = pltpu.get_barrier_semaphore()
    pl.semaphore_signal(barrier, inc=1, device_id=(g, partner), device_id_type=MESH)
    for d in range(2):
        @pl.when(has_link(d))
        def _():
            pl.semaphore_signal(barrier, inc=1, device_id=(g, neighbour(d)), device_id_type=MESH)
    pl.semaphore_wait(barrier, jnp.where(end, 2, 3))

    for d in range(2):
        @pl.when(has_link(d))
        def _():
            send_own(0, d)
    for h in range(2):
        d2d(0, z, h, own=True).start()
    local(wd_ref, wd_v, misc_s.at[0]).start()
    local(wi_ref, wi_v, misc_s.at[1]).start()

    @pl.when(last)
    def _():
        send_own(1, 0)

    @pl.when(first)
    def _():
        send_own(1, 1)

    for h in range(2):
        d2d(1, z, h, own=True).start()
    process(z, own=True)
    copy = local(x_ref, fin_v, misc_s.at[3])
    copy.start()
    copy.wait()
    copy = local(fin_v, xf_ref.at[block(z, c)], misc_s.at[3])
    copy.start()
    copy.wait()
    for h in range(2):
        for d in range(2):
            @pl.when(arrives(d, 0))
            def _():
                arrival(0, d, 0, h)

    @pl.when(z == 2)
    def _():
        send_own(1, 0)

    @pl.when(z == 1)
    def _():
        send_own(1, 1)

    def near(i, _):
        process(jnp.where(first, 1, jnp.where(last, 2, z - 1 + 2 * i)))
        return 0

    lax.fori_loop(0, jnp.where(end, 1, 2), near, 0)

    for h in range(2):
        for d in range(2):
            @pl.when(arrives(d, 1))
            def _():
                arrival(0, d, 1, h)

    @pl.when(z == 1)
    def _():
        send_own(1, 0)

    @pl.when(z == 2)
    def _():
        send_own(1, 1)

    def x_in(zz, d, s):
        @pl.when(z == zz)
        def _():
            for h in range(2):
                arrival(1, d, s, h)

    process(jnp.where(z < 2, z + 2, z - 2))

    @pl.when(end)
    def _():
        sum_at(main, 2, rs_v.at[0])
        rs(0, rs_v.at[0], onward).start()

    x_in(1, 1, 0)
    x_in(2, 0, 0)

    @pl.when(end)
    def _():
        for h in range(2):
            for d in range(2):
                @pl.when(arrives(d, 2))
                def _():
                    arrival(0, d, 2, h)
        process(3 - z)
        sum_at(main, 3, rs_v.at[1])
        rs(1, rs_v.at[1], onward).start()
        sum_at(main, 1, fin_v)
        rs(3, fin_v, onward).start()

    x_in(1, 0, 0)
    x_in(2, 1, 0)

    @pl.when(mid)
    def _():
        sum_at(main, 1, fin_v, 0)
        rs(4, fin_v.at[pl.ds(part, rows - part)], onward).start()
        mid_copy.start()

    pieces = list(range(ff // tile(ff)))
    dw_down_rows(pieces.pop(0))

    x_in(1, 0, 1)
    x_in(2, 1, 1)
    x_in(0, 0, 0)
    x_in(3, 1, 0)

    @pl.when(mid)
    def _():
        sum_at(main, 2, rs_v.at[0], 1)
        rs(2, rs_v.at[0], onward).start()

    if pieces:
        dw_down_rows(pieces.pop(0))
    x_in(0, 0, 1)
    x_in(3, 1, 1)
    while pieces:
        dw_down_rows(pieces.pop(0))

    @pl.when(mid)
    def _():
        sum_at(other, 1, rs_v.at[1], 2)
        hi_copy.start()

        @pl.when(early)
        def _():
            rs(5, rs_v.at[1, pl.ds(0, part)], back).start()

        @pl.when(jnp.logical_not(early))
        def _():
            lo_copy.start()

        for k in (3, 4):
            rs(k).wait_recv()
        base([lin_v.at[3]], lin_v.at[4])

    @pl.when(end)
    def _():
        base([])

    push(z).wait_send()

    @pl.when(mid | jnp.logical_not(early))
    def _():
        out_v[pl.ds(0, part), :] = jnp.zeros((part, d_model), BF16)
        zero_copy.start()

    x_in(0, 0, 2)
    x_in(3, 1, 2)

    for zb in range(CHIPS):
        for h in range(2):
            d2d(1, zb, h, core=1 - c).wait_recv()
            for a in range(2):
                d2d(a, zb, h).wait_send()
    for a in range(2):
        for d in range(2):
            for s in range(3):
                sent = has_link(d) if s == 0 else has_link(d) & arrives(d, s - 1)

                @pl.when(sent)
                def _():
                    for h in range(2):
                        link(a, d, s, h, z).wait_send()

    @pl.when(mid | jnp.logical_not(early))
    def _():
        zero_copy.wait()

    @pl.when(end)
    def _():
        for k, src in ((0, rs_v.at[0]), (1, rs_v.at[1]), (3, fin_v)):
            rs(k, src).wait_send()

        @pl.when(early)
        def _():
            rs(5).wait_recv()

    @pl.when(mid)
    def _():
        for k in (2, 4):
            rs(k).wait_send()
        hi_copy.wait()
        mid_copy.wait()

        @pl.when(early)
        def _():
            rs(5).wait_send()

        @pl.when(jnp.logical_not(early))
        def _():
            lo_copy.wait()

    local(base_v, base_ref, misc_s.at[4]).wait()
    for b in range(2 * CHIPS):
        dpre_out(b).wait()
    for m in range(ff // tile(ff)):
        dw_down_out(m).wait()


def gather_and_sum(dy, x, pre, w_in, w_down):
    rows, d_model = dy.shape
    tokens, ff = pre.shape
    out = jax.ShapeDtypeStruct
    dma = pltpu.SemaphoreType.DMA
    part = max(16, rows * 7 // 22 // 16 * 16)
    flops = 6 * tokens * d_model * ff
    return pl.pallas_call(
        kernel,
        out_shape=(out((tokens, d_model), BF16), out((tokens, d_model), BF16), out((tokens, ff), BF16),
                   out((rows - part, d_model), BF16), out((part, d_model), BF16), out((part, d_model), BF16),
                   out((part, d_model), BF16), out((rows, d_model), F32),
                   out((ff, d_model), BF16)),
        in_specs=[pl.BlockSpec(memory_space=pl.ANY)] * 5,
        out_specs=(pl.BlockSpec(memory_space=pl.ANY),) * 9,
        scratch_shapes=[
            pltpu.VMEM((ff, d_model), BF16),
            pltpu.VMEM((d_model, ff), BF16),
            pltpu.VMEM((tokens, ff), BF16),
            pltpu.VMEM((2, rows, d_model), BF16),
            pltpu.VMEM((2, rows, ff), BF16),
            pltpu.VMEM((CHIPS, rows, d_model), BF16),
            pltpu.VMEM((5, rows, d_model), BF16),
            pltpu.VMEM((rows, d_model), BF16),
            pltpu.VMEM((2, rows, d_model), BF16),
            pltpu.VMEM((rows, d_model), BF16),
            pltpu.VMEM((max(rows, tile(ff)), d_model), F32),
            dma((2, 2, 3, 2)), dma((2, 2, 3, 2)), dma((2, CHIPS, 2)), dma((2, CHIPS, 2)),
            dma, dma((CHIPS,)), dma((6,)), dma((6,)), dma((2, 2)), dma((2 * CHIPS,)), dma((6,)), dma((ff // tile(ff),)),
        ],
        compiler_params=pltpu.CompilerParams(
            collective_id=0, has_side_effects=True, vmem_limit_bytes=66_000_000),
        cost_estimate=pl.CostEstimate(flops=flops, bytes_accessed=8 * tokens * d_model, transcendentals=0),
        name="gather_and_sum",
    )(dy, x, pre, w_in, w_down)


def copy_kernel(src, dst):
    dst[...] = src[...]


def copied(a):
    rows, cols = a.shape
    block = pl.BlockSpec((rows // 9 if rows % 9 == 0 else rows, cols), lambda i: (i, 0))
    return pl.pallas_call(
        copy_kernel, out_shape=jax.ShapeDtypeStruct(a.shape, a.dtype), grid=(9 if rows % 9 == 0 else 1,),
        in_specs=[block], out_specs=block,
        cost_estimate=pl.CostEstimate(flops=rows * cols * 500, bytes_accessed=4 * rows * cols, transcendentals=0),
        compiler_params=pltpu.CompilerParams(vmem_limit_bytes=16_000_000), name="copied")(a)


def solution(mesh):
    def step(x, dy, pre, w_in, w_down):
        _, xf, d_pre, hi, lo, mid, early, base, dw_down = gather_and_sum(dy, x, pre, w_in, w_down)
        hi = lax.ppermute(hi, "tp", [(2, 0), (3, 1), (4, 6), (5, 7)])
        lo = lax.ppermute(lo, "tp", [(2, 0), (4, 6)])
        mid = lax.ppermute(mid, "tp", [(2, 4), (3, 5), (4, 2), (5, 3)])
        dw_down = copied(dw_down)
        dw_in = lax.dot_general(xf, d_pre, TN, preferred_element_type=F32).astype(BF16)
        lo = early.astype(F32) + lo.astype(F32) + mid.astype(F32)
        dx = (base + jnp.concatenate([lo, hi.astype(F32)])).astype(BF16)
        return dx, dw_in, dw_down

    rows = P(("dp", "tp"), None)
    return jax.shard_map(
        step, mesh=mesh,
        in_specs=(rows, rows, P("dp", "tp"), P(None, "tp"), P("tp", None)),
        out_specs=(rows, P("dp", "tp"), rows), check_vma=False)
```

```python
import jax
import jax.numpy as jnp
from jax import lax
from jax.experimental import pallas as pl
from jax.experimental.pallas import tpu as pltpu
from jax.sharding import PartitionSpec as P

MESH = pl.DeviceIdType.MESH
F32, BF16 = jnp.float32, jnp.bfloat16
NT = (((1,), (1,)), ((), ()))
TN = (((0,), (0,)), ((), ()))
CHIPS = 4


def tile(n):
    return next(t for t in (384, 256, 128) if n % t == 0)


def kernel(
    dy_ref, x_ref, pre_ref, wi_ref, wd_ref,
    dyf_ref, xf_ref, dpre_ref, hi_ref, lo2_ref, lo_ref, mid_ref, early_ref, base_lo_ref, base_hi_ref, dwd_ref,
    wd_v, wi_v, dp_v, dyb, preb, prt_v, lin_v, out_v, rs_v, fin_v, acc_v,
    link_s, link_r, d2d_s, d2d_r, push_s, push_r, rs_s, rs_r, load_s, dpre_s, misc_s, dwd_s, ready_s,
):
    me = lax.axis_index("tp")
    g = lax.axis_index("dp")
    z, c = me // 2, me % 2
    rows, d_model = dy_ref.shape
    short = max(16, rows * 2 // 11 // 16 * 16)
    part = early_ref.shape[0]
    cut = base_lo_ref.shape[0]
    sizes = ((rows // 2, rows - rows // 2), (rows - short, short))
    ff = wd_ref.shape[0]
    ins, fulls = (dy_ref, x_ref), (dyf_ref, xf_ref)
    first, last = z == 0, z == CHIPS - 1
    end, mid = (z == 0) | (z == 3), (z == 1) | (z == 2)
    partner = 2 * z + 1 - c

    def block(zb, core):
        return pl.ds(pl.multiple_of((2 * zb + core) * rows, 16), rows)

    def half_of(a, zb, core, h):
        return pl.ds(pl.multiple_of((2 * zb + core) * rows + h * sizes[a][0], 16), sizes[a][h])

    def neighbour(d):
        return 2 * (z - 1 if d == 0 else z + 1) + c

    def link(a, d, s, h, zb, own=False, to=None):
        dst = fulls[a].at[half_of(a, zb, c, h)]
        src = ins[a].at[pl.ds(h * sizes[a][0], sizes[a][h])] if own else dst
        return pltpu.make_async_remote_copy(
            src_ref=src, dst_ref=dst, send_sem=link_s.at[a, d, s, h], recv_sem=link_r.at[a, d, s, h],
            device_id=(g, neighbour(d) if to is None else to), device_id_type=MESH)

    def d2d(a, zb, h, own=False, core=None):
        core = c if core is None else core
        dst = fulls[a].at[half_of(a, zb, core, h)]
        src = ins[a].at[pl.ds(h * sizes[a][0], sizes[a][h])] if own else dst
        return pltpu.make_async_remote_copy(
            src_ref=src, dst_ref=dst, send_sem=d2d_s.at[a, zb, h], recv_sem=d2d_r.at[a, zb, h],
            device_id=(g, partner), device_id_type=MESH)

    def has_link(d):
        return z >= 1 if d == 0 else z <= 2

    def arrives(d, s):
        return z + s + 1 <= 3 if d == 0 else z - s - 1 >= 0

    def source(d, s):
        return z + s + 1 if d == 0 else z - s - 1

    def arrival(a, d, s, h):
        zb = source(d, s)
        link(a, d, s, h, zb, to=partner).wait_recv()
        if s < 2:
            @pl.when(has_link(d))
            def _():
                link(a, d, s + 1, h, zb).start()
        d2d(a, zb, h).start()

    def send_own(a, d):
        for h in range(2):
            link(a, d, 0, h, z, own=True).start()

    def push(zb):
        return pltpu.make_async_remote_copy(
            src_ref=out_v, dst_ref=prt_v.at[zb], send_sem=push_s, recv_sem=push_r.at[zb],
            device_id=(g, partner), device_id_type=MESH)

    def rs(k, src=None, to=None):
        dst = {4: lin_v.at[4, pl.ds(part, rows - part)], 5: early_ref, 6: lin_v.at[4, pl.ds(0, part)]}.get(k)
        dst = lin_v.at[k] if dst is None else dst
        return pltpu.make_async_remote_copy(
            src_ref=dst if src is None else src, dst_ref=dst, send_sem=rs_s.at[k], recv_sem=rs_r.at[k],
            device_id=(g, partner if to is None else to), device_id_type=MESH)

    def local(src, dst, sem):
        return pltpu.make_async_copy(src, dst, sem)

    def dpre_block(slot, b):
        t = tile(ff)
        at = pl.ds(pl.multiple_of(b * rows, 16), rows)

        def body(j, _):
            cols = pl.ds(pl.multiple_of(j * t, 128), t)
            dh = lax.dot_general(dyb[slot], wd_v[cols, :], NT, preferred_element_type=F32)
            p = preb[slot, :, cols].astype(F32)
            dp_v[at, cols] = jnp.where(p > 0, dh * (2.0 * p), 0.0).astype(BF16)
            return 0

        lax.fori_loop(0, ff // t, body, 0)

    def dx_block(b, store, adds, tail=None):
        t = tile(d_model)
        at = pl.ds(pl.multiple_of(b * rows, 16), rows)

        def body(j, _):
            cols = pl.ds(pl.multiple_of(j * t, 128), t)
            acc = lax.dot_general(dp_v[at, :], wi_v[cols, :], NT, preferred_element_type=F32)
            for add in adds:
                acc = acc + add[:, cols].astype(F32)
            store[:, cols] = acc.astype(store.dtype)
            if tail is not None:
                store[pl.ds(part, rows - part), cols] += tail[pl.ds(part, rows - part), cols].astype(F32)
            return 0

        lax.fori_loop(0, d_model // t, body, 0)

    def dpre_out(b):
        at = pl.ds(pl.multiple_of(b * rows, 16), rows)
        return local(dp_v.at[at], dpre_ref.at[at], dpre_s.at[b])

    def load(slot, zb, core, src=None):
        at = block(zb, core)
        return (local(dyf_ref.at[at] if src is None else src, dyb.at[slot], load_s.at[slot, 0]),
                local(pre_ref.at[at], preb.at[slot], load_s.at[slot, 1]))

    def process(zb, own=False):
        for copy in load(0, zb, c, dy_ref if own else None):
            copy.start()
        for h in range(2):
            d2d(0, zb, h, core=1 - c).wait_recv()
        for copy in load(1, zb, 1 - c):
            copy.start()
        if own:
            local(wd_ref, wd_v, misc_s.at[0]).wait()
        for slot in range(2):
            for copy in load(slot, zb, c if slot == 0 else 1 - c, dy_ref if own and slot == 0 else None):
                copy.wait()
            b = 2 * zb + (c if slot == 0 else 1 - c)
            dpre_block(slot, b)
            dpre_out(b).start()
        if own:
            local(dyb.at[0], dyf_ref.at[block(z, c)], misc_s.at[2]).start()
            local(wi_ref, wi_v, misc_s.at[1]).wait()
            local(dyb.at[0], dyf_ref.at[block(z, c)], misc_s.at[2]).wait()
        else:
            push(zb).wait_send()
        dx_block(2 * zb + 1 - c, out_v, ())
        push(zb).start()

    def dw_down_rows(m):
        t, tn = tile(ff), 512 if d_model % 512 == 0 else tile(d_model)
        cols = pl.ds(m * t, t)

        def loads(b, slot):
            at = pl.ds(pl.multiple_of(b * rows, 16), rows)
            return (local(dyf_ref.at[at], dyb.at[slot], load_s.at[slot, 0]),
                    local(pre_ref.at[at, cols], preb.at[slot, :, pl.ds(0, t)], load_s.at[slot, 1]))

        for copy in loads(0, 0):
            copy.start()
        acc_v[...] = jnp.zeros_like(acc_v)

        def token_block(b, _):
            slot = b % 2

            @pl.when(b + 1 < 2 * CHIPS)
            def _():
                for copy in loads(b + 1, 1 - slot):
                    copy.start()

            for copy in loads(b, slot):
                copy.wait()
            hidden = jnp.square(jnp.maximum(preb[slot, :, pl.ds(0, t)].astype(F32), 0.0)).astype(BF16)

            def body(n, _):
                at = pl.ds(pl.multiple_of(n * tn, 128), tn)
                acc_v[:, at] += lax.dot_general(hidden, dyb[slot, :, at], TN, preferred_element_type=F32)
                return 0

            return lax.fori_loop(0, d_model // tn, body, 0)

        lax.fori_loop(0, 2 * CHIPS, token_block, 0)

        def body(n, _):
            at = pl.ds(pl.multiple_of(n * tn, 128), tn)
            wd_v[cols, at] = acc_v[:, at].astype(BF16)
            return 0

        lax.fori_loop(0, d_model // tn, body, 0)
        dw_down_out(m).start()

    def dw_down_out(m):
        at = pl.ds(m * tile(ff), tile(ff))
        return local(wd_v.at[at], dwd_ref.at[at], dwd_s.at[m])

    main = jnp.where(z >= 2, 0, 1)
    other = 1 - main

    def chip_at(d, s):
        return z + s * (2 * d - 1)

    def sum_at(d, s, store, lin=None):
        zb = chip_at(d, s)
        push(zb).wait_recv()
        adds = [prt_v.at[zb]]
        if lin is not None:
            rs(lin).wait_recv()
            adds.append(lin_v.at[lin])
        dx_block(2 * zb + c, store, adds)

    def base(adds, tail=None):
        push(z).wait_recv()
        dx_block(2 * z + c, base_v, [prt_v.at[z]] + adds, tail)
        for copy in base_copies():
            copy.start()

    base_v = acc_v.at[pl.ds(0, rows)]

    def base_copies():
        return (local(acc_v.at[pl.ds(0, cut)], base_lo_ref, misc_s.at[4]),
                local(acc_v.at[pl.ds(cut, rows - cut)], base_hi_ref, misc_s.at[2]))

    onward, back = 2 * chip_at(main, 1) + c, 2 * chip_at(other, 1) + c
    early = c == 1
    hi_copy = local(rs_v.at[1, pl.ds(cut, rows - cut)], hi_ref, misc_s.at[3])
    lo2_copy = local(rs_v.at[1, pl.ds(part, cut - part)], lo2_ref, load_s.at[0, 0])
    lo_copy = local(rs_v.at[1, pl.ds(0, part)], lo_ref, misc_s.at[0])
    mid_copy = local(fin_v.at[pl.ds(0, part)], mid_ref, misc_s.at[1])
    zero_copy = local(out_v.at[pl.ds(0, part)], early_ref, misc_s.at[5])

    barrier = pltpu.get_barrier_semaphore()
    pl.semaphore_signal(barrier, inc=1, device_id=(g, partner), device_id_type=MESH)

    @pl.when((z == 1) | last)
    def _():
        pl.semaphore_signal(barrier, inc=1, device_id=(g, neighbour(0)), device_id_type=MESH)

    @pl.when(has_link(1))
    def _():
        pl.semaphore_signal(barrier, inc=1, device_id=(g, neighbour(1)), device_id_type=MESH)

    pl.semaphore_wait(barrier, jnp.where(z == 2, 3, 2))

    @pl.when(has_link(0))
    def _():
        send_own(0, 0)

    for h in range(2):
        d2d(0, z, h, own=True).start()

    @pl.when(z == 2)
    def _():
        pl.semaphore_signal(ready_s, inc=1, device_id=(g, neighbour(0)), device_id_type=MESH)

    @pl.when(z == 1)
    def _():
        pl.semaphore_wait(ready_s, 1)

    @pl.when(has_link(1))
    def _():
        send_own(0, 1)

    local(wd_ref, wd_v, misc_s.at[0]).start()
    local(wi_ref, wi_v, misc_s.at[1]).start()

    @pl.when(last)
    def _():
        send_own(1, 0)

    @pl.when(first)
    def _():
        send_own(1, 1)

    for h in range(2):
        d2d(1, z, h, own=True).start()
    process(z, own=True)
    copy = local(x_ref, fin_v, misc_s.at[3])
    copy.start()
    copy.wait()
    copy = local(fin_v, xf_ref.at[block(z, c)], misc_s.at[3])
    copy.start()
    copy.wait()
    for h in range(2):
        for d in range(2):
            @pl.when(arrives(d, 0))
            def _():
                arrival(0, d, 0, h)

    @pl.when(z == 2)
    def _():
        send_own(1, 0)

    @pl.when(z == 1)
    def _():
        send_own(1, 1)

    def near(i, _):
        process(jnp.where(first, 1, jnp.where(last, 2, z - 1 + 2 * i)))
        return 0

    lax.fori_loop(0, jnp.where(end, 1, 2), near, 0)

    for h in range(2):
        for d in range(2):
            @pl.when(arrives(d, 1))
            def _():
                arrival(0, d, 1, h)

    @pl.when(z == 1)
    def _():
        send_own(1, 0)

    @pl.when(z == 2)
    def _():
        send_own(1, 1)

    def x_in(zz, d, s):
        @pl.when(z == zz)
        def _():
            for h in range(2):
                arrival(1, d, s, h)

    process(jnp.where(z < 2, z + 2, z - 2))

    @pl.when(end)
    def _():
        sum_at(main, 2, rs_v.at[0])
        rs(0, rs_v.at[0], onward).start()

    x_in(1, 1, 0)
    x_in(2, 0, 0)

    @pl.when(end)
    def _():
        for h in range(2):
            for d in range(2):
                @pl.when(arrives(d, 2))
                def _():
                    arrival(0, d, 2, h)
        process(3 - z)
        sum_at(main, 3, rs_v.at[1])
        rs(1, rs_v.at[1], onward).start()
        sum_at(main, 1, fin_v)
        rs(3, fin_v, onward).start()

    x_in(1, 0, 0)
    x_in(2, 1, 0)

    @pl.when(mid)
    def _():
        sum_at(main, 1, fin_v, 0)
        rs(4, fin_v.at[pl.ds(part, rows - part)], onward).start()

    pieces = list(range(ff // tile(ff)))
    dw_down_rows(pieces.pop(0))

    x_in(1, 0, 1)
    x_in(2, 1, 1)
    x_in(0, 0, 0)
    x_in(3, 1, 0)

    @pl.when(mid)
    def _():
        sum_at(main, 2, rs_v.at[0], 1)
        rs(2, rs_v.at[0], onward).start()

        @pl.when(early)
        def _():
            rs(6, fin_v.at[pl.ds(0, part)], onward).start()

        @pl.when(jnp.logical_not(early))
        def _():
            mid_copy.start()

    if pieces:
        dw_down_rows(pieces.pop(0))
    x_in(0, 0, 1)
    x_in(3, 1, 1)
    while pieces:
        dw_down_rows(pieces.pop(0))

    @pl.when(mid)
    def _():
        sum_at(other, 1, rs_v.at[1], 2)
        hi_copy.start()
        lo2_copy.start()

        @pl.when(early)
        def _():
            rs(5, rs_v.at[1, pl.ds(0, part)], back).start()

        @pl.when(jnp.logical_not(early))
        def _():
            lo_copy.start()

        for k in (3, 4):
            rs(k).wait_recv()

        @pl.when(early)
        def _():
            rs(6).wait_recv()
            base([lin_v.at[3], lin_v.at[4]])

        @pl.when(jnp.logical_not(early))
        def _():
            base([lin_v.at[3]], lin_v.at[4])

    @pl.when(end)
    def _():
        base([])

    push(z).wait_send()

    @pl.when(mid | jnp.logical_not(early))
    def _():
        out_v[pl.ds(0, part), :] = jnp.zeros((part, d_model), BF16)
        zero_copy.start()

    x_in(0, 0, 2)
    x_in(3, 1, 2)

    for zb in range(CHIPS):
        for h in range(2):
            d2d(1, zb, h, core=1 - c).wait_recv()
            for a in range(2):
                d2d(a, zb, h).wait_send()
    for a in range(2):
        for d in range(2):
            for s in range(3):
                sent = has_link(d) if s == 0 else has_link(d) & arrives(d, s - 1)

                @pl.when(sent)
                def _():
                    for h in range(2):
                        link(a, d, s, h, z).wait_send()

    @pl.when(mid | jnp.logical_not(early))
    def _():
        zero_copy.wait()

    @pl.when(end)
    def _():
        for k, src in ((0, rs_v.at[0]), (1, rs_v.at[1]), (3, fin_v)):
            rs(k, src).wait_send()

        @pl.when(early)
        def _():
            rs(5).wait_recv()

    @pl.when(mid)
    def _():
        for k in (2, 4):
            rs(k).wait_send()
        hi_copy.wait()
        lo2_copy.wait()

        @pl.when(early)
        def _():
            rs(5).wait_send()
            rs(6).wait_send()

        @pl.when(jnp.logical_not(early))
        def _():
            lo_copy.wait()
            mid_copy.wait()

    for copy in base_copies():
        copy.wait()
    for b in range(2 * CHIPS):
        dpre_out(b).wait()
    for m in range(ff // tile(ff)):
        dw_down_out(m).wait()


def gather_and_sum(dy, x, pre, w_in, w_down):
    rows, d_model = dy.shape
    tokens, ff = pre.shape
    out = jax.ShapeDtypeStruct
    dma = pltpu.SemaphoreType.DMA
    part = max(16, rows * 8 // 22 // 16 * 16)
    cut = rows - max(16, rows * 2 // 11 // 16 * 16)
    flops = 6 * tokens * d_model * ff
    return pl.pallas_call(
        kernel,
        out_shape=(out((tokens, d_model), BF16), out((tokens, d_model), BF16), out((tokens, ff), BF16),
                   out((rows - cut, d_model), BF16), out((cut - part, d_model), BF16), out((part, d_model), BF16),
                   out((part, d_model), BF16), out((part, d_model), BF16), out((cut, d_model), F32),
                   out((rows - cut, d_model), F32),
                   out((ff, d_model), BF16)),
        in_specs=[pl.BlockSpec(memory_space=pl.ANY)] * 5,
        out_specs=(pl.BlockSpec(memory_space=pl.ANY),) * 11,
        scratch_shapes=[
            pltpu.VMEM((ff, d_model), BF16),
            pltpu.VMEM((d_model, ff), BF16),
            pltpu.VMEM((tokens, ff), BF16),
            pltpu.VMEM((2, rows, d_model), BF16),
            pltpu.VMEM((2, rows, ff), BF16),
            pltpu.VMEM((CHIPS, rows, d_model), BF16),
            pltpu.VMEM((5, rows, d_model), BF16),
            pltpu.VMEM((rows, d_model), BF16),
            pltpu.VMEM((2, rows, d_model), BF16),
            pltpu.VMEM((rows, d_model), BF16),
            pltpu.VMEM((max(rows, tile(ff)), d_model), F32),
            dma((2, 2, 3, 2)), dma((2, 2, 3, 2)), dma((2, CHIPS, 2)), dma((2, CHIPS, 2)),
            dma, dma((CHIPS,)), dma((7,)), dma((7,)), dma((2, 2)), dma((2 * CHIPS,)), dma((6,)), dma((ff // tile(ff),)), pltpu.SemaphoreType.REGULAR,
        ],
        compiler_params=pltpu.CompilerParams(
            collective_id=0, has_side_effects=True, vmem_limit_bytes=66_000_000),
        cost_estimate=pl.CostEstimate(flops=flops, bytes_accessed=8 * tokens * d_model, transcendentals=0),
        name="gather_and_sum",
    )(dy, x, pre, w_in, w_down)


def dw_in_kernel(x_ref, d_pre_ref, dwd_ref, dw_in_ref, out_ref):
    dw_in_ref[...] = lax.dot_general(x_ref[...], d_pre_ref[...], TN, preferred_element_type=F32).astype(BF16)
    out_ref[...] = dwd_ref[...]


def dw_in_and_copy(x, d_pre, dw_down):
    tokens, d_model = x.shape
    ff = d_pre.shape[1]
    t = 512 if d_model % 512 == 0 else tile(d_model)
    n = d_model // t
    rows = pl.BlockSpec((ff // n, d_model), lambda i: (i, 0))
    return pl.pallas_call(
        dw_in_kernel, grid=(n,),
        out_shape=(jax.ShapeDtypeStruct((d_model, ff), BF16), jax.ShapeDtypeStruct((ff, d_model), BF16)),
        in_specs=[pl.BlockSpec((tokens, t), lambda i: (0, i)),
                  pl.BlockSpec((tokens, ff), lambda i: (0, 0), pipeline_mode=pl.Buffered(1)), rows],
        out_specs=(pl.BlockSpec((t, ff), lambda i: (i, 0)), rows),
        cost_estimate=pl.CostEstimate(flops=2 * tokens * d_model * ff, bytes_accessed=4 * tokens * d_model, transcendentals=0),
        compiler_params=pltpu.CompilerParams(vmem_limit_bytes=58_000_000))(x, d_pre, dw_down)


def first_rows_kernel(base_ref, early_ref, lo_ref, mid_ref, lo2_ref, dx_ref):
    cut, d_model = base_ref.shape
    part, t = early_ref.shape[0], tile(d_model)
    low, high = pl.ds(0, part), pl.ds(part, cut - part)

    def body(j, _):
        at = pl.ds(pl.multiple_of(j * t, 128), t)
        total = base_ref[low, at]
        for ref in (early_ref, lo_ref, mid_ref):
            total = total + ref[:, at].astype(F32)
        dx_ref[low, at] = total.astype(BF16)
        dx_ref[high, at] = (base_ref[high, at] + lo2_ref[:, at].astype(F32)).astype(BF16)
        return 0

    lax.fori_loop(0, d_model // t, body, 0)


def first_rows(rows, base, *adds):
    def whole(a):
        return pl.BlockSpec(a.shape, lambda i: (0, 0), pipeline_mode=pl.Buffered(1))

    return pl.pallas_call(
        first_rows_kernel, grid=(1,), out_shape=jax.ShapeDtypeStruct((rows, base.shape[1]), BF16),
        in_specs=[whole(a) for a in (base, *adds)], out_specs=pl.BlockSpec(base.shape, lambda i: (0, 0)),
        cost_estimate=pl.CostEstimate(flops=4 * rows * base.shape[1], bytes_accessed=12 * base.size, transcendentals=0),
        compiler_params=pltpu.CompilerParams(vmem_limit_bytes=40_000_000), name="first_rows")(base, *adds)


def solution(mesh):
    def step(x, dy, pre, w_in, w_down):
        _, xf, d_pre, hi, lo2, lo, mid, early, base_lo, base_hi, dw_down = gather_and_sum(dy, x, pre, w_in, w_down)
        to_ends = [(2, 0), (3, 1), (4, 6), (5, 7)]
        lo = lax.ppermute(lo, "tp", [(2, 0), (4, 6)])
        lo2 = lax.ppermute(lo2, "tp", to_ends)
        hi = lax.ppermute(hi, "tp", to_ends)
        mid = lax.ppermute(mid, "tp", [(2, 4), (4, 2)])
        dw_in, dw_down = dw_in_and_copy(xf, d_pre, dw_down)
        dx = first_rows(dy.shape[0], base_lo, early, lo, mid, lo2)
        hi = (base_hi + hi.astype(F32)).astype(BF16)
        dx = lax.dynamic_update_slice(dx, hi, (base_lo.shape[0], 0))
        return dx, dw_in, dw_down

    rows = P(("dp", "tp"), None)
    return jax.shard_map(
        step, mesh=mesh,
        in_specs=(rows, rows, P("dp", "tp"), P(None, "tp"), P("tp", None)),
        out_specs=(rows, P("dp", "tp"), rows), check_vma=False)
```
